32 devices in a mesh: ctx: 2 (over x), grp: 4 (over y, core), tp: 4 (over z).
Axes of the slice: x: 2, y: 2, z: 4, core: 2. Of those that a mesh axis runs over, the one named last changes fastest.
Arguments:
- tokens: bfloat16 [4096, 4608], P(('grp', 'ctx')), parts along dimension 0, may hold values from -6 to 6
- token_pos: int32 [4096], P(('grp', 'ctx')), parts along dimension 0, may hold values from 0 to 1023, as said below
- norm_gain: float32 [4608], replicated, may hold values from 0.1 to 1.9
- query_weight: bfloat16 [4608, 4096], P('ctx', 'tp'), may hold values from -0.09375 to 0.09375
- key_weight: bfloat16 [4608, 2048], P('ctx', 'tp'), may hold values from -0.09375 to 0.09375
- value_weight: bfloat16 [4608, 2048], P('ctx', 'tp'), may hold values from -0.09375 to 0.09375
Outputs:
- attended: bfloat16 [4096, 4096], P(('grp', 'ctx'), 'tp'), parts along dimension 0
The draws below stay inside these ranges and needn't reach their ends.
There are 4 independent parts, one for each index of `grp`. The reference program is written for one: setup_inputs(seed, part) draws one part's arguments, and reference() takes and returns one part's arrays. A program takes and returns all parts, laid end to end along the dimension named above; an argument that names none is the same for every part. Nothing has to cross between parts.
Inputs may be any that keep to these rules, and one draw needn't show every extreme that they name: `token_pos`: the 512 rows of each index of ctx form two runs of 256 consecutive ascending positions, each starting at a multiple of 256; every position of the sequence occurs exactly once.
All inputs are finite; a program needn't handle non-finite values.
Results may differ from the reference program's by a relative error of at most 0.0077.
Values may be sent and summed in bfloat16 or wider, within the bound.
A program may use at most 128 MiB of HBM per device.

```python
import jax
import jax.numpy as jnp
from jax import lax

D = 4608
HEADS = 32
KV_HEADS = 16
HEAD_DIM = 128
TOK_DEV = 512
TOKENS = 1024


def draw_token_pos(key, part):
    half = TOK_DEV // 2
    devices = TOKENS // TOK_DEV
    blocks = 2 * devices
    order = jax.random.permutation(jax.random.fold_in(key, 12), blocks).astype(jnp.int32)
    target = (jnp.asarray(part).astype(jnp.int32) % blocks).astype(jnp.int32)
    where_target = jnp.argmax((order == target).astype(jnp.int32)).astype(jnp.int32)
    leading = order[0]
    order = order.at[where_target].set(leading)
    order = order.at[0].set(target)
    starts = order * half
    positions = starts[:, None] + jnp.arange(half, dtype=jnp.int32)[None, :]
    return positions.reshape(-1).astype(jnp.int32)


def levels(own_key, shape, shards, smallest, largest):
    def one(axis_at, shards_of):
        steps = jax.random.uniform(jax.random.fold_in(jax.random.fold_in(own_key, 6), axis_at), (shards_of,), jnp.float32, smallest / len(shards), largest / len(shards))
        return jnp.repeat(jnp.exp(steps), shape[axis_at] // shards_of).reshape((-1,) + (1,) * (len(shape) - axis_at - 1))

    factor_of = one(*shards[0])
    for cut in shards[1:]:
        factor_of = factor_of * one(*cut)
    return factor_of


def normal_values(key, shape, spread, reach, split=(), held_as=jnp.bfloat16):
    result = spread * jax.random.normal(key, shape, jnp.float32)
    if split:
        result = result * levels(key, shape, split, -0.22, 0.18)
    return jnp.clip(result, -reach, reach).astype(held_as)


def setup_inputs(seed: int = 0, part: int = 0) -> dict:
    seeds = jax.random.split(jax.random.key(seed), 7)
    own_keys = jax.random.split(jax.random.fold_in(seeds[6], part), 7)
    tokens = normal_values(own_keys[0], (TOKENS, D), 1.0, 6.0, ((0, 2),))
    token_pos = draw_token_pos(jax.random.fold_in(jax.random.fold_in(seeds[6], part), 71), part)
    norm_gain = jnp.clip(1.0 + 0.18 * jax.random.normal(seeds[2], (D,), jnp.float32), 0.1, 1.9)
    query_weight = normal_values(seeds[3], (D, HEADS * HEAD_DIM), D ** -0.5, 0.09375, ((0, 2), (1, 4)))
    key_weight = normal_values(seeds[4], (D, KV_HEADS * HEAD_DIM), D ** -0.5, 0.09375, ((0, 2), (1, 4)))
    value_weight = normal_values(seeds[5], (D, KV_HEADS * HEAD_DIM), D ** -0.5, 0.09375, ((0, 2), (1, 4)))
    return {"tokens": tokens, "token_pos": token_pos, "norm_gain": norm_gain, "query_weight": query_weight, "key_weight": key_weight, "value_weight": value_weight}


query_scale = 144.0 ** (-0.5)

def rotate(field, positions):
    half = field.shape[-1] // 2
    freq = 10000.0 ** (-jnp.arange(half, dtype=jnp.float32) * 2.0 / field.shape[-1])
    angle = positions.astype(jnp.float32)[:, None] * freq[None, :]
    cosine = jnp.cos(angle)[:, None, :]
    sine = jnp.sin(angle)[:, None, :]
    first = field[..., :half]
    second = field[..., half:]
    return jnp.concatenate([first * cosine - second * sine, second * cosine + first * sine], -1)

def reference(tokens, token_pos, norm_gain, query_weight, key_weight, value_weight):
    count = tokens.shape[0]
    inputs = tokens.astype(jnp.float32)
    normed = (inputs * lax.rsqrt(lax.optimization_barrier(jnp.mean(inputs * inputs, -1, keepdims=True)) + 1e-06) * norm_gain[None, :]).astype(jnp.bfloat16)
    queries = jnp.dot(normed, query_weight, preferred_element_type=jnp.float32).reshape(count, HEADS, HEAD_DIM)
    queries = (rotate(queries, token_pos) * query_scale).astype(jnp.bfloat16)
    keys = jnp.dot(normed, key_weight, preferred_element_type=jnp.float32).reshape(count, KV_HEADS, HEAD_DIM)
    keys = rotate(keys, token_pos).astype(jnp.bfloat16)
    values = jnp.dot(normed, value_weight, preferred_element_type=jnp.float32).astype(jnp.bfloat16)
    values = values.reshape(count, KV_HEADS, HEAD_DIM)
    key_full = lax.optimization_barrier(keys).astype(jnp.float32)
    value_full = lax.optimization_barrier(values).astype(jnp.float32)
    half = TOK_DEV // 2
    query_blocks = queries.reshape(count // half, half, KV_HEADS, 2, HEAD_DIM)
    pos_blocks = token_pos.reshape(count // half, half)

    def block(args):
        query_part, pos_part = args
        query_part = lax.optimization_barrier(query_part).astype(jnp.float32)
        scores = jnp.einsum('ngrd,mgd->grnm', query_part, key_full)
        capped = 50.0 * jnp.tanh(scores / 50.0)
        allowed = token_pos[None, None, None, :] <= pos_part[None, None, :, None]
        weights = jnp.where(allowed, jnp.exp(capped), 0.0).astype(jnp.bfloat16)
        weights = lax.optimization_barrier(weights).astype(jnp.float32)
        numerator = jnp.einsum('grnm,mgd->ngrd', weights, value_full)
        total = lax.optimization_barrier(jnp.sum(weights, -1))
        return (numerator / jnp.transpose(total, (2, 0, 1))[..., None]).astype(jnp.bfloat16)
    attended = lax.map(block, (query_blocks, pos_blocks))
    return attended.reshape(count, HEADS * HEAD_DIM)
```

```python
import functools
import math

import jax
import jax.numpy as jnp
from jax import lax
from jax.experimental import pallas as pl
from jax.experimental.pallas import tpu as pltpu
from jax.sharding import PartitionSpec as P

HEAD_DIM = 128
BLOCK = 2 * HEAD_DIM
MESH = pl.DeviceIdType.MESH

query_scale = 144.0 ** (-0.5)


def each(start, stop, body):
    if stop - start == 1:
        body(start)
    elif stop > start:
        lax.fori_loop(start, stop, lambda i, _: (body(i), None)[1], None)


def kernel(
    n, grp, pos_ref, freq_ref, gain_ref, tok_ref, q_ref, k_ref, v_ref, out_ref,
    wbuf, normed, kvbuf, posbuf, qbuf, acc, cos_ref, sin_ref, qpos_ref,
    tok_sem, own_sem, x_send, x_recv, y_send, y_recv, s_send, s_recv, t_send, t_recv,
    kv_send, kv_recv, pos_send, pos_recv,
):
    c = lax.axis_index("ctx")
    g = lax.axis_index("grp")
    pairs = grp // 2
    near = g % 2
    pair = g // 2
    sibling = pair * 2 + (1 - near)
    depth = q_ref.shape[0]
    part = depth // grp
    rows = tok_ref.shape[0]
    kv_blocks = k_ref.shape[1] // BLOCK
    q_blocks = q_ref.shape[1] // BLOCK
    sources = [(k_ref, i) for i in range(kv_blocks)]
    sources += [(v_ref, i) for i in range(kv_blocks)]
    sources += [(q_ref, i) for i in range(q_blocks)]
    blocks = len(sources)

    def region(owner, member):
        return pl.ds(pl.multiple_of(owner * depth + member * part, 16), part)

    def peer(d):
        return lax.rem(c + d, n)

    def source(d):
        return lax.rem(c + n - d, n)

    def far(j):
        return lax.rem(pair + j, pairs)

    def near_of(j):
        return lax.rem(pair + pairs - j, pairs)

    def x_copy(b, d):
        ref, col = sources[b]
        return pltpu.make_async_remote_copy(
            src_ref=ref.at[pl.ds(pl.multiple_of(g * part, 16), part), pl.ds(col * BLOCK, BLOCK)],
            dst_ref=wbuf.at[b, region(c, g)],
            send_sem=x_send.at[b, d - 1], recv_sem=x_recv.at[b, d - 1],
            device_id={"ctx": peer(d)}, device_id_type=MESH,
        )

    def hop(b, where, send, recv, member):
        return pltpu.make_async_remote_copy(
            src_ref=wbuf.at[b, where], dst_ref=wbuf.at[b, where],
            send_sem=send, recv_sem=recv, device_id={"grp": member}, device_id_type=MESH,
        )

    def y_copy(b, d, j):
        return hop(b, region(source(d), g), y_send.at[b, d - 1, j - 1], y_recv.at[b, d - 1, j - 1],
                   far(j) * 2 + near)

    def y_wait(b, d, j):
        hop(b, region(source(d), near_of(j) * 2 + near), y_send.at[b, d - 1, j - 1],
            y_recv.at[b, d - 1, j - 1], sibling).wait_recv()

    def s_copy(b, d):
        return hop(b, region(source(d), g), s_send.at[b, d - 1], s_recv.at[b, d - 1], sibling)

    def s_wait(b, d):
        hop(b, region(source(d), sibling), s_send.at[b, d - 1], s_recv.at[b, d - 1],
            sibling).wait_recv()

    def t_copy(b, d, j):
        return hop(b, region(source(d), near_of(j) * 2 + near), t_send.at[b, d - 1, j - 1],
                   t_recv.at[b, d - 1, j - 1], sibling)

    def t_wait(b, d, j):
        hop(b, region(source(d), near_of(j) * 2 + 1 - near), t_send.at[b, d - 1, j - 1],
            t_recv.at[b, d - 1, j - 1], sibling).wait_recv()

    def kv_copy(b, d, owner):
        return pltpu.make_async_remote_copy(
            src_ref=kvbuf.at[b, owner], dst_ref=kvbuf.at[b, owner],
            send_sem=kv_send.at[b, d - 1], recv_sem=kv_recv.at[b, d - 1],
            device_id={"ctx": peer(d)}, device_id_type=MESH,
        )

    def pos_copy(d, owner):
        return pltpu.make_async_remote_copy(
            src_ref=pos_ref, dst_ref=posbuf.at[owner],
            send_sem=pos_send.at[d - 1], recv_sem=pos_recv.at[d - 1],
            device_id={"ctx": peer(d)}, device_id_type=MESH,
        )

    def own_copy(b):
        ref, col = sources[b]
        return pltpu.make_async_copy(
            ref.at[:, pl.ds(col * BLOCK, BLOCK)],
            wbuf.at[b, pl.ds(pl.multiple_of(c * depth, 16), depth)], own_sem.at[b],
        )

    tok_copy = pltpu.make_async_copy(tok_ref, normed, tok_sem)
    tok_copy.start()

    barrier = pltpu.get_barrier_semaphore()

    def greet(**where):
        pl.semaphore_signal(barrier, inc=1, device_id=where, device_id_type=MESH)

    each(1, n, lambda d: greet(ctx=peer(d)))
    each(1, pairs, lambda j: greet(grp=far(j) * 2 + near))
    greet(grp=sibling)
    pl.semaphore_wait(barrier, n - 1 + pairs - 1 + 1)

    def send_block(b):
        each(1, n, lambda d: x_copy(b, d).start())

    send_block(0)
    each(1, n, lambda d: pos_copy(d, c).start())
    send_block(1)
    for b in range(blocks):
        own_copy(b).start()

    posbuf[c] = pos_ref[...]
    qpos = jnp.transpose(
        jnp.broadcast_to(pos_ref[0:1, :].astype(jnp.float32), (HEAD_DIM, rows)), (1, 0)
    )
    qpos_ref[...] = qpos
    angle = qpos * freq_ref[...]
    lane = lax.broadcasted_iota(jnp.int32, angle.shape, 1)
    sine = jnp.sin(angle)
    cos_ref[...] = jnp.cos(angle)
    sin_ref[...] = jnp.where(lane < HEAD_DIM // 2, -sine, sine)

    tok_copy.wait()
    strip = 32

    def norm_rows(i):
        where = pl.ds(pl.multiple_of(i * strip, strip), strip)
        inputs = normed[where, :].astype(jnp.float32)
        mean = jnp.mean(inputs * inputs, -1, keepdims=True)
        normed[where, :] = (inputs * lax.rsqrt(mean + 1e-06) * gain_ref[...]).astype(jnp.bfloat16)

    each(0, rows // strip, norm_rows)

    tall = math.gcd(rows, 256)

    def project(b, target, rope, scale):
        def tile(i):
            where = pl.ds(pl.multiple_of(i * tall, tall), tall)
            field = jnp.dot(normed[where, :], wbuf[b], preferred_element_type=jnp.float32)
            if rope:
                cosine, sine = cos_ref[where, :], sin_ref[where, :]
                halves = []
                for h in range(2):
                    one = field[:, h * HEAD_DIM : (h + 1) * HEAD_DIM]
                    halves.append(one * cosine + pltpu.roll(one, HEAD_DIM // 2, 1) * sine)
                field = jnp.concatenate(halves, -1)
            if scale is not None:
                field = field * scale
            target[where, :] = field.astype(jnp.bfloat16)

        each(0, rows // tall, tile)

    def attend(b, owner, first, last):
        piece, col = b // 2, (b % 2) * HEAD_DIM

        def tile(i):
            where = pl.ds(pl.multiple_of(i * tall, tall), tall)
            keys = kvbuf[piece, owner, :, pl.ds(col, HEAD_DIM)]
            values = kvbuf[kv_blocks + piece, owner, :, pl.ds(col, HEAD_DIM)]
            values = jnp.concatenate([values, jnp.ones_like(values)], -1)
            key_pos = posbuf[owner, 0:1, :].astype(jnp.float32)
            allowed = key_pos <= qpos_ref[where, 0:1]
            for h in range(2):
                cols = pl.ds(h * HEAD_DIM, HEAD_DIM)
                scores = lax.dot_general(
                    qbuf[b, where, cols], keys, (((1,), (1,)), ((), ())),
                    preferred_element_type=jnp.float32,
                )
                capped = jnp.tanh(scores * (1.0 / 50.0)) * (50.0 * math.log2(math.e))
                weights = jnp.where(allowed, jnp.exp2(capped), 0.0).astype(jnp.bfloat16)
                both = jnp.dot(weights, values, preferred_element_type=jnp.float32)
                if not first:
                    both = both + acc[b, h, where, :]
                if last:
                    done = both[:, :HEAD_DIM] / both[:, HEAD_DIM:]
                    out_ref[where, pl.ds(b * BLOCK + h * HEAD_DIM, HEAD_DIM)] = done.astype(
                        out_ref.dtype
                    )
                else:
                    acc[b, h, where, :] = both

        each(0, rows // tall, tile)

    received = set()

    def attend_others(b):
        piece = b // 2
        if "pos" not in received:
            received.add("pos")
            each(1, n, lambda d: pos_copy(d, source(d)).wait_recv())
        for index in (piece, kv_blocks + piece):
            if index not in received:
                received.add(index)
                each(1, n, lambda d: kv_copy(index, d, source(d)).wait_recv())
        each(1, n - 1, lambda d: attend(b, source(d), False, False))
        attend(b, source(n - 1), False, True)

    def send_kv(b):
        each(1, n, lambda d: kv_copy(b, d, c).start())

    for t in range(blocks + 2):
        if t < blocks:
            def forward(d, b=t):
                x_copy(b, d).wait_recv()
                each(1, pairs, lambda j: y_copy(b, d, j).start())
                s_copy(b, d).start()

            each(1, n, forward)
        if 1 <= t <= blocks:
            def onward(d, b=t - 1):
                def one(j):
                    y_wait(b, d, j)
                    t_copy(b, d, j).start()

                each(1, pairs, one)

            each(1, n, onward)
        if t >= 2:
            b = t - 2

            def arrive(d, b=b):
                s_wait(b, d)
                each(1, pairs, lambda j: t_wait(b, d, j))

            each(1, n, arrive)
            own_copy(b).wait()
            if b < 2 * kv_blocks:
                project(b, kvbuf.at[b, c], b < kv_blocks, None)
        if 3 <= t <= 2 * kv_blocks + 2:
            send_kv(t - 3)
        if t + 2 < blocks:
            send_block(t + 2)
        if t >= 2 and t - 2 >= 2 * kv_blocks:
            h = t - 2 - 2 * kv_blocks
            project(t - 2, qbuf.at[h], True, query_scale)
            attend(h, c, True, False)
            if h > 0:
                attend_others(h - 1)
    attend_others(q_blocks - 1)

    def settle(d):
        pos_copy(d, c).wait_send()
        for b in range(2 * kv_blocks):
            kv_copy(b, d, c).wait_send()
        for b in range(blocks):
            x_copy(b, d).wait_send()
            s_copy(b, d).wait_send()

            def pair_sends(j, b=b):
                y_copy(b, d, j).wait_send()
                t_copy(b, d, j).wait_send()

            each(1, pairs, pair_sends)

    each(1, n, settle)


def on_device(n, grp, tokens, token_pos, norm_gain, query_weight, key_weight, value_weight):
    rows, width = tokens.shape
    depth, q_cols = query_weight.shape
    kv_cols = key_weight.shape[1]
    q_blocks, kv_blocks = q_cols // BLOCK, kv_cols // BLOCK
    blocks = q_blocks + 2 * kv_blocks
    pairs = grp // 2
    half = HEAD_DIM // 2
    freq = 10000.0 ** (-jnp.arange(half, dtype=jnp.float32) * 2.0 / HEAD_DIM)
    freq = jnp.concatenate([freq, freq])[None, :]
    pos = jnp.broadcast_to(token_pos[None, :], (8, rows))
    dma = pltpu.SemaphoreType.DMA
    far = max(pairs - 1, 1)
    vmem = pl.BlockSpec(memory_space=pltpu.VMEM)
    anywhere = pl.BlockSpec(memory_space=pl.ANY)
    return pl.pallas_call(
        functools.partial(kernel, n, grp),
        out_shape=jax.ShapeDtypeStruct((rows, q_cols), jnp.bfloat16),
        in_specs=[vmem] * 3 + [anywhere] * 4,
        out_specs=vmem,
        scratch_shapes=[
            pltpu.VMEM((blocks, n * depth, BLOCK), jnp.bfloat16),
            pltpu.VMEM((rows, width), jnp.bfloat16),
            pltpu.VMEM((2 * kv_blocks, n, rows, BLOCK), jnp.bfloat16),
            pltpu.VMEM((n, 8, rows), jnp.int32),
            pltpu.VMEM((q_blocks, rows, BLOCK), jnp.bfloat16),
            pltpu.VMEM((q_blocks, 2, rows, BLOCK), jnp.float32),
            pltpu.VMEM((rows, HEAD_DIM), jnp.float32),
            pltpu.VMEM((rows, HEAD_DIM), jnp.float32),
            pltpu.VMEM((rows, HEAD_DIM), jnp.float32),
            dma(()),
            dma((blocks,)),
            dma((blocks, n - 1)),
            dma((blocks, n - 1)),
            dma((blocks, n - 1, far)),
            dma((blocks, n - 1, far)),
            dma((blocks, n - 1)),
            dma((blocks, n - 1)),
            dma((blocks, n - 1, far)),
            dma((blocks, n - 1, far)),
            dma((2 * kv_blocks, n - 1)),
            dma((2 * kv_blocks, n - 1)),
            dma((n - 1,)),
            dma((n - 1,)),
        ],
        compiler_params=pltpu.CompilerParams(
            collective_id=0, has_side_effects=True, vmem_limit_bytes=64 * 1024 * 1024 - 65536
        ),
    )(pos, freq, norm_gain[None, :], tokens, query_weight, key_weight, value_weight)


def solution(mesh):
    in_specs = (
        P(("grp", "ctx"), None),
        P(("grp", "ctx")),
        P(),
        P("ctx", "tp"),
        P("ctx", "tp"),
        P("ctx", "tp"),
    )
    out_specs = P(("grp", "ctx"), "tp")
    return jax.shard_map(
        functools.partial(on_device, mesh.shape["ctx"], mesh.shape["grp"]),
        mesh=mesh, in_specs=in_specs, out_specs=out_specs, check_vma=False,
    )
```

```python
import functools
import math

import jax
import jax.numpy as jnp
import numpy as np
from jax import lax
from jax.experimental import pallas as pl
from jax.experimental.pallas import tpu as pltpu
from jax.sharding import PartitionSpec as P

HEAD_DIM = 128
BLOCK = 2 * HEAD_DIM
MESH = pl.DeviceIdType.MESH

query_scale = 144.0 ** (-0.5)


def each(start, stop, body):
    if stop - start == 1:
        body(start)
    elif stop > start:
        lax.fori_loop(start, stop, lambda i, _: (body(i), None)[1], None)


def kernel(
    n, grp, pos_ref, freq_ref, gain_ref, tok_ref, q_ref, k_ref, v_ref, out_ref,
    wbuf, normed, kvbuf, posbuf, qbuf, acc, cos_ref, sin_ref, qpos_ref,
    tok_sem, own_sem, x_send, x_recv, y_send, y_recv, s_send, s_recv, t_send, t_recv,
    kv_send, kv_recv, pos_send, pos_recv,
):
    c = lax.axis_index("ctx")
    g = lax.axis_index("grp")
    pairs = grp // 2
    near = g % 2
    pair = g // 2
    sibling = pair * 2 + (1 - near)
    depth = q_ref.shape[0]
    part = depth // grp
    rows = tok_ref.shape[0]
    kv_blocks = k_ref.shape[1] // BLOCK
    groups = k_ref.shape[1] // HEAD_DIM
    q_blocks = q_ref.shape[1] // BLOCK
    sources = [(k_ref, i) for i in range(kv_blocks)]
    sources += [(v_ref, i) for i in range(kv_blocks)]
    sources += [(q_ref, i) for i in range(q_blocks)]
    blocks = len(sources)

    def region(owner, member):
        return pl.ds(pl.multiple_of(owner * depth + member * part, 16), part)

    def peer(d):
        return lax.rem(c + d, n)

    def source(d):
        return lax.rem(c + n - d, n)

    def far(j):
        return lax.rem(pair + j, pairs)

    def near_of(j):
        return lax.rem(pair + pairs - j, pairs)

    def x_copy(b, d):
        ref, col = sources[b]
        return pltpu.make_async_remote_copy(
            src_ref=ref.at[pl.ds(pl.multiple_of(g * part, 16), part), pl.ds(col * BLOCK, BLOCK)],
            dst_ref=wbuf.at[b, region(c, g)],
            send_sem=x_send.at[b, d - 1], recv_sem=x_recv.at[b, d - 1],
            device_id={"ctx": peer(d)}, device_id_type=MESH,
        )

    def hop(b, where, send, recv, member):
        return pltpu.make_async_remote_copy(
            src_ref=wbuf.at[b, where], dst_ref=wbuf.at[b, where],
            send_sem=send, recv_sem=recv, device_id={"grp": member}, device_id_type=MESH,
        )

    def y_copy(b, d, j):
        return hop(b, region(source(d), g), y_send.at[b, d - 1, j - 1], y_recv.at[b, d - 1, j - 1],
                   far(j) * 2 + near)

    def y_wait(b, d, j):
        hop(b, region(source(d), near_of(j) * 2 + near), y_send.at[b, d - 1, j - 1],
            y_recv.at[b, d - 1, j - 1], sibling).wait_recv()

    def s_copy(b, d):
        return hop(b, region(source(d), g), s_send.at[b, d - 1], s_recv.at[b, d - 1], sibling)

    def s_wait(b, d):
        hop(b, region(source(d), sibling), s_send.at[b, d - 1], s_recv.at[b, d - 1],
            sibling).wait_recv()

    def t_copy(b, d, j):
        return hop(b, region(source(d), near_of(j) * 2 + near), t_send.at[b, d - 1, j - 1],
                   t_recv.at[b, d - 1, j - 1], sibling)

    def t_wait(b, d, j):
        hop(b, region(source(d), near_of(j) * 2 + 1 - near), t_send.at[b, d - 1, j - 1],
            t_recv.at[b, d - 1, j - 1], sibling).wait_recv()

    def kv_copy(b, d, owner):
        return pltpu.make_async_remote_copy(
            src_ref=kvbuf.at[b, owner], dst_ref=kvbuf.at[b, owner],
            send_sem=kv_send.at[b, d - 1], recv_sem=kv_recv.at[b, d - 1],
            device_id={"ctx": peer(d)}, device_id_type=MESH,
        )

    def pos_copy(d, owner):
        return pltpu.make_async_remote_copy(
            src_ref=posbuf.at[owner], dst_ref=posbuf.at[owner],
            send_sem=pos_send.at[d - 1], recv_sem=pos_recv.at[d - 1],
            device_id={"ctx": peer(d)}, device_id_type=MESH,
        )

    def own_copy(b):
        ref, col = sources[b]
        return pltpu.make_async_copy(
            ref.at[:, pl.ds(col * BLOCK, BLOCK)],
            wbuf.at[b, pl.ds(pl.multiple_of(c * depth, 16), depth)], own_sem.at[b],
        )

    tok_copy = pltpu.make_async_copy(tok_ref, normed, tok_sem)
    tok_copy.start()

    barrier = pltpu.get_barrier_semaphore()

    def greet(**where):
        pl.semaphore_signal(barrier, inc=1, device_id=where, device_id_type=MESH)

    each(1, n, lambda d: greet(ctx=peer(d)))
    each(1, pairs, lambda j: greet(grp=far(j) * 2 + near))
    greet(grp=sibling)
    pl.semaphore_wait(barrier, n - 1 + pairs - 1 + 1)

    def send_block(b):
        each(1, n, lambda d: x_copy(b, d).start())

    send_block(0)
    send_block(1)
    for b in range(blocks):
        own_copy(b).start()

    lanes = pos_ref[...][None, :]
    posbuf[c] = jnp.broadcast_to(lanes, posbuf.shape[1:])
    qpos = jnp.transpose(
        jnp.broadcast_to(lanes.astype(jnp.float32), (HEAD_DIM, rows)), (1, 0)
    )
    qpos_ref[...] = qpos
    angle = qpos * freq_ref[...]
    lane = lax.broadcasted_iota(jnp.int32, angle.shape, 1)
    sine = jnp.sin(angle)
    cos_ref[...] = jnp.cos(angle)
    sin_ref[...] = jnp.where(lane < HEAD_DIM // 2, -sine, sine)

    tok_copy.wait()
    strip = 32

    def norm_rows(i):
        where = pl.ds(pl.multiple_of(i * strip, strip), strip)
        inputs = normed[where, :].astype(jnp.float32)
        mean = jnp.mean(inputs * inputs, -1, keepdims=True)
        normed[where, :] = (inputs * lax.rsqrt(mean + 1e-06) * gain_ref[...][None, :]).astype(jnp.bfloat16)

    each(0, rows // strip, norm_rows)

    tall = math.gcd(rows, 256)

    def project(b, store, rope, scale):
        def tile(i):
            where = pl.ds(pl.multiple_of(i * tall, tall), tall)
            field = jnp.dot(normed[where, :], wbuf[b], preferred_element_type=jnp.float32)
            if rope:
                cosine, sine = cos_ref[where, :], sin_ref[where, :]
                halves = []
                for h in range(2):
                    one = field[:, h * HEAD_DIM : (h + 1) * HEAD_DIM]
                    halves.append(one * cosine + pltpu.roll(one, HEAD_DIM // 2, 1) * sine)
                field = jnp.concatenate(halves, -1)
            if scale is not None:
                field = field * scale
            store(where, field.astype(jnp.bfloat16))

        each(0, rows // tall, tile)

    def attend(b, owner, first, last):
        def tile(i):
            where = pl.ds(pl.multiple_of(i * tall, tall), tall)
            keys = kvbuf[b, owner]
            values = kvbuf[groups + b, owner]
            values = jnp.concatenate([values, jnp.ones_like(values)], -1)
            key_pos = posbuf[owner, 0:1, :].astype(jnp.float32)
            allowed = key_pos <= qpos_ref[where, 0:1]
            for h in range(2):
                cols = pl.ds(h * HEAD_DIM, HEAD_DIM)
                scores = lax.dot_general(
                    qbuf[b, where, cols], keys, (((1,), (1,)), ((), ())),
                    preferred_element_type=jnp.float32,
                )
                capped = jnp.tanh(scores * (1.0 / 50.0)) * (50.0 * math.log2(math.e))
                weights = jnp.where(allowed, jnp.exp2(capped), 0.0).astype(jnp.bfloat16)
                both = jnp.dot(weights, values, preferred_element_type=jnp.float32)
                if not first:
                    both = both + acc[b, h, where, :]
                if last:
                    done = both[:, :HEAD_DIM] / both[:, HEAD_DIM:]
                    out_ref[where, pl.ds(b * BLOCK + h * HEAD_DIM, HEAD_DIM)] = done.astype(
                        out_ref.dtype
                    )
                else:
                    acc[b, h, where, :] = both

        each(0, rows // tall, tile)

    received = set()

    def attend_others(b):
        if "pos" not in received:
            received.add("pos")
            each(1, n, lambda d: pos_copy(d, source(d)).wait_recv())
        for index in (b, groups + b):
            if index not in received:
                received.add(index)
                each(1, n, lambda d: kv_copy(index, d, source(d)).wait_recv())
        each(1, n - 1, lambda d: attend(b, source(d), False, False))
        attend(b, source(n - 1), False, True)

    def send_group(h):
        each(1, n, lambda d: kv_copy(h, d, c).start())
        each(1, n, lambda d: kv_copy(groups + h, d, c).start())

    def store_kv(first):
        def store(where, field):
            kvbuf[first, c, where, :] = field[:, :HEAD_DIM]
            kvbuf[first + 1, c, where, :] = field[:, HEAD_DIM:]

        return store

    def store_q(h):
        def store(where, field):
            qbuf[h, where, :] = field

        return store

    for t in range(blocks + 2):
        if t < blocks:
            def forward(d, b=t):
                x_copy(b, d).wait_recv()
                each(1, pairs, lambda j: y_copy(b, d, j).start())
                s_copy(b, d).start()

            each(1, n, forward)
        if 1 <= t <= blocks:
            def onward(d, b=t - 1):
                def one(j):
                    y_wait(b, d, j)
                    t_copy(b, d, j).start()

                each(1, pairs, one)

            each(1, n, onward)
        if t >= 2:
            b = t - 2

            def arrive(d, b=b):
                s_wait(b, d)
                each(1, pairs, lambda j: t_wait(b, d, j))

            each(1, n, arrive)
            own_copy(b).wait()
            if b < 2 * kv_blocks:
                project(b, store_kv(2 * b), b < kv_blocks, None)
        if t + 2 < blocks:
            send_block(t + 2)
        if t == 2:
            each(1, n, lambda d: pos_copy(d, c).start())
        if t >= blocks - 2:
            share = [h for h in range(groups) if min(blocks - 2 + h, blocks) == t]
            for h in share:
                send_group(h)
        if t >= 2 and t - 2 >= 2 * kv_blocks:
            h = t - 2 - 2 * kv_blocks
            project(t - 2, store_q(h), True, query_scale)
            attend(h, c, True, False)
            if t == blocks:
                attend_others(0)
    for h in range(1, q_blocks):
        attend_others(h)

    def settle(d):
        pos_copy(d, c).wait_send()
        for b in range(2 * groups):
            kv_copy(b, d, c).wait_send()
        for b in range(blocks):
            x_copy(b, d).wait_send()
            s_copy(b, d).wait_send()

            def pair_sends(j, b=b):
                y_copy(b, d, j).wait_send()
                t_copy(b, d, j).wait_send()

            each(1, pairs, pair_sends)

    each(1, n, settle)


def on_device(n, grp, tokens, token_pos, norm_gain, query_weight, key_weight, value_weight):
    rows, width = tokens.shape
    depth, q_cols = query_weight.shape
    kv_cols = key_weight.shape[1]
    q_blocks, kv_blocks = q_cols // BLOCK, kv_cols // BLOCK
    blocks = q_blocks + 2 * kv_blocks
    pairs = grp // 2
    half = HEAD_DIM // 2
    freq = 10000.0 ** (-np.arange(half) * 2.0 / HEAD_DIM)
    freq = np.concatenate([freq, freq])[None, :].astype(np.float32)
    dma = pltpu.SemaphoreType.DMA
    far = max(pairs - 1, 1)
    vmem = pl.BlockSpec(memory_space=pltpu.VMEM)
    anywhere = pl.BlockSpec(memory_space=pl.ANY)
    return pl.pallas_call(
        functools.partial(kernel, n, grp),
        out_shape=jax.ShapeDtypeStruct((rows, q_cols), jnp.bfloat16),
        in_specs=[vmem] * 3 + [anywhere] * 4,
        out_specs=vmem,
        scratch_shapes=[
            pltpu.VMEM((blocks, n * depth, BLOCK), jnp.bfloat16),
            pltpu.VMEM((rows, width), jnp.bfloat16),
            pltpu.VMEM((4 * kv_blocks, n, rows, HEAD_DIM), jnp.bfloat16),
            pltpu.VMEM((n, 8, rows), jnp.int32),
            pltpu.VMEM((q_blocks, rows, BLOCK), jnp.bfloat16),
            pltpu.VMEM((q_blocks, 2, rows, BLOCK), jnp.float32),
            pltpu.VMEM((rows, HEAD_DIM), jnp.float32),
            pltpu.VMEM((rows, HEAD_DIM), jnp.float32),
            pltpu.VMEM((rows, HEAD_DIM), jnp.float32),
            dma(()),
            dma((blocks,)),
            dma((blocks, n - 1)),
            dma((blocks, n - 1)),
            dma((blocks, n - 1, far)),
            dma((blocks, n - 1, far)),
            dma((blocks, n - 1)),
            dma((blocks, n - 1)),
            dma((blocks, n - 1, far)),
            dma((blocks, n - 1, far)),
            dma((4 * kv_blocks, n - 1)),
            dma((4 * kv_blocks, n - 1)),
            dma((n - 1,)),
            dma((n - 1,)),
        ],
        compiler_params=pltpu.CompilerParams(
            collective_id=0, has_side_effects=True, vmem_limit_bytes=64 * 1024 * 1024 - 65536
        ),
    )(token_pos, freq, norm_gain, tokens, query_weight, key_weight, value_weight)


def solution(mesh):
    in_specs = (
        P(("grp", "ctx"), None),
        P(("grp", "ctx")),
        P(),
        P("ctx", "tp"),
        P("ctx", "tp"),
        P("ctx", "tp"),
    )
    out_specs = P(("grp", "ctx"), "tp")
    return jax.shard_map(
        functools.partial(on_device, mesh.shape["ctx"], mesh.shape["grp"]),
        mesh=mesh, in_specs=in_specs, out_specs=out_specs, check_vma=False,
    )
```

```python
import functools
import math

import jax
import jax.numpy as jnp
import numpy as np
from jax import lax
from jax.experimental import pallas as pl
from jax.experimental.pallas import tpu as pltpu
from jax.sharding import PartitionSpec as P

HEAD_DIM = 128
BLOCK = 2 * HEAD_DIM
MESH = pl.DeviceIdType.MESH

query_scale = 144.0 ** (-0.5)


def each(start, stop, body):
    if stop - start == 1:
        body(start)
    elif stop > start:
        lax.fori_loop(start, stop, lambda i, _: (body(i), None)[1], None)


def kernel(
    n, grp, pos_ref, freq_ref, gain_ref, tok_ref, q_ref, k_ref, v_ref, out_ref,
    wbuf, normed, kvbuf, posbuf, qbuf, acc, cos_ref, sin_ref, qpos_ref,
    tok_sem, own_sem, x_send, x_recv, y_send, y_recv, s_send, s_recv, t_send, t_recv,
    kv_send, kv_recv, pos_send, pos_recv,
):
    c = lax.axis_index("ctx")
    g = lax.axis_index("grp")
    pairs = grp // 2
    near = g % 2
    pair = g // 2
    sibling = pair * 2 + (1 - near)
    depth = q_ref.shape[0]
    part = depth // grp
    rows = tok_ref.shape[0]
    kv_blocks = k_ref.shape[1] // BLOCK
    groups = k_ref.shape[1] // HEAD_DIM
    q_blocks = q_ref.shape[1] // BLOCK
    sources = [(k_ref, i) for i in range(kv_blocks)]
    sources += [(v_ref, i) for i in range(kv_blocks)]
    sources += [(q_ref, i) for i in range(q_blocks)]
    blocks = len(sources)

    def region(owner, member):
        return pl.ds(pl.multiple_of(owner * depth + member * part, 16), part)

    def peer(d):
        return lax.rem(c + d, n)

    def source(d):
        return lax.rem(c + n - d, n)

    def far(j):
        return lax.rem(pair + j, pairs)

    def near_of(j):
        return lax.rem(pair + pairs - j, pairs)

    def x_copy(b, d):
        return pltpu.make_async_remote_copy(
            src_ref=wbuf.at[b, region(c, g)], dst_ref=wbuf.at[b, region(c, g)],
            send_sem=x_send.at[b, d - 1], recv_sem=x_recv.at[b, d - 1],
            device_id={"ctx": peer(d)}, device_id_type=MESH,
        )

    def hop(b, where, send, recv, member):
        return pltpu.make_async_remote_copy(
            src_ref=wbuf.at[b, where], dst_ref=wbuf.at[b, where],
            send_sem=send, recv_sem=recv, device_id={"grp": member}, device_id_type=MESH,
        )

    def y_copy(b, d, j):
        return hop(b, region(source(d), g), y_send.at[b, d - 1, j - 1], y_recv.at[b, d - 1, j - 1],
                   far(j) * 2 + near)

    def y_wait(b, d, j):
        hop(b, region(source(d), near_of(j) * 2 + near), y_send.at[b, d - 1, j - 1],
            y_recv.at[b, d - 1, j - 1], sibling).wait_recv()

    def s_copy(b, d):
        return hop(b, region(source(d), g), s_send.at[b, d - 1], s_recv.at[b, d - 1], sibling)

    def s_wait(b, d):
        hop(b, region(source(d), sibling), s_send.at[b, d - 1], s_recv.at[b, d - 1],
            sibling).wait_recv()

    def t_copy(b, d, j):
        return hop(b, region(source(d), near_of(j) * 2 + near), t_send.at[b, d - 1, j - 1],
                   t_recv.at[b, d - 1, j - 1], sibling)

    def t_wait(b, d, j):
        hop(b, region(source(d), near_of(j) * 2 + 1 - near), t_send.at[b, d - 1, j - 1],
            t_recv.at[b, d - 1, j - 1], sibling).wait_recv()

    def kv_copy(b, d, owner):
        return pltpu.make_async_remote_copy(
            src_ref=kvbuf.at[b, owner], dst_ref=kvbuf.at[b, owner],
            send_sem=kv_send.at[b, d - 1], recv_sem=kv_recv.at[b, d - 1],
            device_id={"ctx": peer(d)}, device_id_type=MESH,
        )

    def pos_copy(d, owner):
        return pltpu.make_async_remote_copy(
            src_ref=posbuf.at[owner], dst_ref=posbuf.at[owner],
            send_sem=pos_send.at[d - 1], recv_sem=pos_recv.at[d - 1],
            device_id={"ctx": peer(d)}, device_id_type=MESH,
        )

    def own_copy(b):
        ref, col = sources[b]
        return pltpu.make_async_copy(
            ref.at[:, pl.ds(col * BLOCK, BLOCK)],
            wbuf.at[b, pl.ds(pl.multiple_of(c * depth, 16), depth)], own_sem.at[b],
        )

    tok_copy = pltpu.make_async_copy(tok_ref, normed, tok_sem)
    own_copy(0).start()
    own_copy(1).start()
    tok_copy.start()
    for b in range(2, blocks):
        own_copy(b).start()

    barrier = pltpu.get_barrier_semaphore()

    def greet(**where):
        pl.semaphore_signal(barrier, inc=1, device_id=where, device_id_type=MESH)

    each(1, n, lambda d: greet(ctx=peer(d)))
    each(1, pairs, lambda j: greet(grp=far(j) * 2 + near))
    greet(grp=sibling)
    pl.semaphore_wait(barrier, n - 1 + pairs - 1 + 1)

    def send_block(b):
        own_copy(b).wait()
        each(1, n, lambda d: x_copy(b, d).start())

    send_block(0)
    send_block(1)

    lanes = pos_ref[...][None, :]
    posbuf[c] = jnp.broadcast_to(lanes, posbuf.shape[1:])
    qpos = jnp.transpose(
        jnp.broadcast_to(lanes.astype(jnp.float32), (HEAD_DIM, rows)), (1, 0)
    )
    qpos_ref[...] = qpos
    angle = qpos * freq_ref[...]
    lane = lax.broadcasted_iota(jnp.int32, angle.shape, 1)
    sine = jnp.sin(angle)
    cos_ref[...] = jnp.cos(angle)
    sin_ref[...] = jnp.where(lane < HEAD_DIM // 2, -sine, sine)

    tok_copy.wait()
    strip = 32

    def norm_rows(i):
        where = pl.ds(pl.multiple_of(i * strip, strip), strip)
        inputs = normed[where, :].astype(jnp.float32)
        mean = jnp.mean(inputs * inputs, -1, keepdims=True)
        normed[where, :] = (inputs * lax.rsqrt(mean + 1e-06) * gain_ref[...][None, :]).astype(jnp.bfloat16)

    each(0, rows // strip, norm_rows)

    tall = math.gcd(rows, 256)

    def project(b, store, rope, scale):
        def tile(i):
            where = pl.ds(pl.multiple_of(i * tall, tall), tall)
            field = jnp.dot(normed[where, :], wbuf[b], preferred_element_type=jnp.float32)
            if rope:
                cosine, sine = cos_ref[where, :], sin_ref[where, :]
                halves = []
                for h in range(2):
                    one = field[:, h * HEAD_DIM : (h + 1) * HEAD_DIM]
                    halves.append(one * cosine + pltpu.roll(one, HEAD_DIM // 2, 1) * sine)
                field = jnp.concatenate(halves, -1)
            if scale is not None:
                field = field * scale
            store(where, field.astype(jnp.bfloat16))

        each(0, rows // tall, tile)

    def attend(b, owner, first, last):
        def tile(i):
            where = pl.ds(pl.multiple_of(i * tall, tall), tall)
            keys = kvbuf[b, owner]
            values = kvbuf[groups + b, owner]
            values = jnp.concatenate([values, jnp.ones_like(values)], -1)
            key_pos = posbuf[owner, 0:1, :].astype(jnp.float32)
            allowed = key_pos <= qpos_ref[where, 0:1]
            for h in range(2):
                cols = pl.ds(h * HEAD_DIM, HEAD_DIM)
                scores = lax.dot_general(
                    qbuf[b, where, cols], keys, (((1,), (1,)), ((), ())),
                    preferred_element_type=jnp.float32,
                )
                capped = jnp.tanh(scores * (1.0 / 50.0)) * (50.0 * math.log2(math.e))
                weights = jnp.where(allowed, jnp.exp2(capped), 0.0).astype(jnp.bfloat16)
                both = jnp.dot(weights, values, preferred_element_type=jnp.float32)
                if not first:
                    both = both + acc[b, h, where, :]
                if last:
                    done = both[:, :HEAD_DIM] / both[:, HEAD_DIM:]
                    out_ref[where, pl.ds(b * BLOCK + h * HEAD_DIM, HEAD_DIM)] = done.astype(
                        out_ref.dtype
                    )
                else:
                    acc[b, h, where, :] = both

        each(0, rows // tall, tile)

    received = set()

    def attend_others(b):
        if "pos" not in received:
            received.add("pos")
            each(1, n, lambda d: pos_copy(d, source(d)).wait_recv())
        for index in (b, groups + b):
            if index not in received:
                received.add(index)
                each(1, n, lambda d: kv_copy(index, d, source(d)).wait_recv())
        each(1, n - 1, lambda d: attend(b, source(d), False, False))
        attend(b, source(n - 1), False, True)

    def send_group(h):
        each(1, n, lambda d: kv_copy(h, d, c).start())
        each(1, n, lambda d: kv_copy(groups + h, d, c).start())

    def store_kv(first):
        def store(where, field):
            kvbuf[first, c, where, :] = field[:, :HEAD_DIM]
            kvbuf[first + 1, c, where, :] = field[:, HEAD_DIM:]

        return store

    def store_q(h):
        def store(where, field):
            qbuf[h, where, :] = field

        return store

    for t in range(blocks + 2):
        if t < blocks:
            def forward(d, b=t):
                x_copy(b, d).wait_recv()
                each(1, pairs, lambda j: y_copy(b, d, j).start())
                s_copy(b, d).start()

            each(1, n, forward)
        if 1 <= t <= blocks:
            def onward(d, b=t - 1):
                def one(j):
                    y_wait(b, d, j)
                    t_copy(b, d, j).start()

                each(1, pairs, one)

            each(1, n, onward)
        if t >= 2:
            b = t - 2

            def arrive(d, b=b):
                s_wait(b, d)
                each(1, pairs, lambda j: t_wait(b, d, j))

            each(1, n, arrive)
            if b < 2 * kv_blocks:
                project(b, store_kv(2 * b), b < kv_blocks, None)
        if t + 2 < blocks:
            send_block(t + 2)
        if t == 2:
            each(1, n, lambda d: pos_copy(d, c).start())
        if t >= blocks - 2:
            share = [h for h in range(groups) if min(blocks - 2 + h, blocks) == t]
            for h in share:
                send_group(h)
        if t >= 2 and t - 2 >= 2 * kv_blocks:
            h = t - 2 - 2 * kv_blocks
            project(t - 2, store_q(h), True, query_scale)
            attend(h, c, True, False)
            if t == blocks:
                attend_others(0)
    for h in range(1, q_blocks):
        attend_others(h)

    def settle(d):
        pos_copy(d, c).wait_send()
        for b in range(2 * groups):
            kv_copy(b, d, c).wait_send()
        for b in range(blocks):
            x_copy(b, d).wait_send()
            s_copy(b, d).wait_send()

            def pair_sends(j, b=b):
                y_copy(b, d, j).wait_send()
                t_copy(b, d, j).wait_send()

            each(1, pairs, pair_sends)

    each(1, n, settle)


def write_out(in_ref, out_ref, sem):
    copy = pltpu.make_async_copy(in_ref, out_ref, sem)
    copy.start()
    copy.wait()


def on_device(n, grp, tokens, token_pos, norm_gain, query_weight, key_weight, value_weight):
    rows, width = tokens.shape
    depth, q_cols = query_weight.shape
    kv_cols = key_weight.shape[1]
    q_blocks, kv_blocks = q_cols // BLOCK, kv_cols // BLOCK
    blocks = q_blocks + 2 * kv_blocks
    pairs = grp // 2
    half = HEAD_DIM // 2
    freq = 10000.0 ** (-np.arange(half) * 2.0 / HEAD_DIM)
    freq = np.concatenate([freq, freq])[None, :].astype(np.float32)
    dma = pltpu.SemaphoreType.DMA
    far = max(pairs - 1, 1)
    vmem = pl.BlockSpec(memory_space=pltpu.VMEM)
    anywhere = pl.BlockSpec(memory_space=pl.ANY)
    held = [pltpu.with_memory_space_constraint(x, pltpu.HBM) for x in (tokens, query_weight, key_weight, value_weight)]
    attended = pl.pallas_call(
        functools.partial(kernel, n, grp),
        out_shape=pltpu.VMEM((rows, q_cols), jnp.bfloat16),
        in_specs=[vmem] * 3 + [pl.BlockSpec(memory_space=pltpu.HBM)] * 4,
        out_specs=vmem,
        scratch_shapes=[
            pltpu.VMEM((blocks, n * depth, BLOCK), jnp.bfloat16),
            pltpu.VMEM((rows, width), jnp.bfloat16),
            pltpu.VMEM((4 * kv_blocks, n, rows, HEAD_DIM), jnp.bfloat16),
            pltpu.VMEM((n, 8, rows), jnp.int32),
            pltpu.VMEM((q_blocks, rows, BLOCK), jnp.bfloat16),
            pltpu.VMEM((q_blocks, 2, rows, BLOCK), jnp.float32),
            pltpu.VMEM((rows, HEAD_DIM), jnp.float32),
            pltpu.VMEM((rows, HEAD_DIM), jnp.float32),
            pltpu.VMEM((rows, HEAD_DIM), jnp.float32),
            dma(()),
            dma((blocks,)),
            dma((blocks, n - 1)),
            dma((blocks, n - 1)),
            dma((blocks, n - 1, far)),
            dma((blocks, n - 1, far)),
            dma((blocks, n - 1)),
            dma((blocks, n - 1)),
            dma((blocks, n - 1, far)),
            dma((blocks, n - 1, far)),
            dma((4 * kv_blocks, n - 1)),
            dma((4 * kv_blocks, n - 1)),
            dma((n - 1,)),
            dma((n - 1,)),
        ],
        compiler_params=pltpu.CompilerParams(
            collective_id=0, has_side_effects=True, vmem_limit_bytes=44 * 1024 * 1024
        ),
    )(token_pos, freq, norm_gain, *held)
    return pl.pallas_call(
        write_out,
        out_shape=jax.ShapeDtypeStruct(attended.shape, attended.dtype),
        in_specs=[vmem],
        out_specs=anywhere,
        scratch_shapes=[dma(())],
        compiler_params=pltpu.CompilerParams(vmem_limit_bytes=4 * 1024 * 1024),
    )(attended)


def solution(mesh):
    in_specs = (
        P(("grp", "ctx"), None),
        P(("grp", "ctx")),
        P(),
        P("ctx", "tp"),
        P("ctx", "tp"),
        P("ctx", "tp"),
    )
    out_specs = P(("grp", "ctx"), "tp")
    return jax.shard_map(
        functools.partial(on_device, mesh.shape["ctx"], mesh.shape["grp"]),
        mesh=mesh, in_specs=in_specs, out_specs=out_specs, check_vma=False,
    )
```
